512 devices in a mesh: vit: 8 (over z_hi, y), seq: 8 (over z_lo), tensor: 8 (over x, core).
Axes of the slice: x: 4, y: 4, z: 16 (z_hi: 2, z_lo: 8; z = z_hi * 8 + z_lo), core: 2. Of those that a mesh axis runs over, the one named last changes fastest.
Arguments:
- merged: bfloat16 [2048, 8192], P(('vit', 'seq'), 'tensor'), may hold values from -6 to 6
- positions: int32 [2048], P(('vit', 'seq')), may hold values from 0 to 131071, as said below
- picked: int32 [2048], P(('vit', 'seq')), may hold values from 0 to 1, as said below
- router_score: float32 [2048], P(('vit', 'seq')), may hold values from -8 to 8
- up_weight: bfloat16 [8192, 16384], P('tensor', ('vit', 'seq')), may hold values from -0.0625 to 0.0625
- down_weight: bfloat16 [16384, 8192], P(('vit', 'seq'), 'tensor'), may hold values from -0.046875 to 0.046875
- mixed_grad: bfloat16 [1024, 8192], P(('vit', 'seq'), 'tensor'), may hold values from -6 to 6
Outputs:
- mixed: bfloat16 [1024, 8192], P(('vit', 'seq'), 'tensor')
- token_grad: bfloat16 [2048, 8192], P(('vit', 'seq'), 'tensor')
- up_grad: float32 [8192, 16384], P('tensor', ('vit', 'seq'))
- down_grad: float32 [16384, 8192], P(('vit', 'seq'), 'tensor')
The draws below stay inside these ranges and needn't reach their ends.
Inputs may be any that keep to these rules, and one draw needn't show every extreme that they name: Among the picked tokens of one aligned block of 32 tokens, at most 2 have the same positions // 16384, and in every block some value of positions // 16384 is shared by exactly 2 picked tokens. `picked`: exactly 8 ones in every aligned block of 32 tokens.
All inputs are finite; a program needn't handle non-finite values.
Results may differ from the reference program's by a relative error of at most 0.0056.
Values may be sent and summed in bfloat16 or wider, within the bound.
A program may use at most 64 MiB of HBM per device.

```python
import jax
import jax.numpy as jnp
from jax import lax

D = 8192
FF = 16384
CAP = 2
SPAN = 16384
VIS_GRP = 32
PICK = 8
GROUPS = 64
VIS = 2048
SLOTS = 1024
N_VIT = 8
N_SEQ = 8


def route_group(key):
    keys = jax.random.split(key, 6)
    slot_count = N_SEQ * CAP
    order = jax.random.permutation(keys[0], VIS_GRP)
    slot_ids = jnp.arange(slot_count, dtype=jnp.int32)
    slot_owner = slot_ids // CAP
    ranking = jax.random.permutation(keys[1], N_SEQ).astype(jnp.int32)
    forced = jax.random.randint(keys[2], (), 0, N_SEQ)
    noise = jax.random.randint(keys[3], (slot_count,), 0, 8192)
    scores = (noise + ranking[slot_owner] * 4096 + (slot_owner == forced).astype(jnp.int32) * 1048576) * slot_count + slot_ids
    unused, chosen = lax.top_k(scores, PICK)
    chosen_owner = slot_owner[chosen]
    free_owner = jax.random.randint(keys[4], (VIS_GRP,), 0, N_SEQ)
    owner = free_owner.at[order[:PICK]].set(chosen_owner)
    chosen_flag = jnp.zeros((VIS_GRP,), jnp.int32).at[order[:PICK]].set(1)
    offset = jax.random.randint(keys[5], (VIS_GRP,), 0, SPAN)
    return (owner * SPAN + offset, chosen_flag)


def route_all(key):
    base = jax.random.fold_in(key, 11)
    keys = jax.random.split(base, N_VIT * N_SEQ)
    spots, flags = jax.vmap(route_group)(keys)
    return (spots.reshape(-1).astype(jnp.int32), flags.reshape(-1).astype(jnp.int32))


def draw_positions(key, part):
    return route_all(key)[0]


def draw_picked(key, part):
    return route_all(key)[1]


def shard_levels(stream_key, dims, pieces, low, largest):
    gain, own = 1.0, jax.random.fold_in(stream_key, 6)
    for dim, parts in pieces:
        draws = jnp.exp(jax.random.uniform(jax.random.fold_in(own, dim), (parts,), jnp.float32, low / len(pieces), largest / len(pieces)))
        gain = gain * jnp.repeat(draws, dims[dim] // parts).reshape([-1 if axis == dim else 1 for axis in range(len(dims))])
    return gain


def gaussian(own_key, dims, spread, bound, pieces=(), held_as=jnp.bfloat16):
    values = spread * jax.random.normal(own_key, dims, jnp.float32)
    if pieces:
        values = values * shard_levels(own_key, dims, pieces, -0.22, 0.18)
    return jnp.clip(values, -bound, bound).astype(held_as)


def setup_inputs(seed: int = 0) -> dict:
    splits = jax.random.split(jax.random.key(seed), 8)
    return {
        "merged": gaussian(splits[0], (VIS, D), 1.0, 6.0, ((0, 64), (1, 8))),
        "positions": draw_positions(jax.random.fold_in(splits[7], 71), 0),
        "picked": draw_picked(jax.random.fold_in(splits[7], 71), 0),
        "router_score": gaussian(splits[3], (VIS,), 2.0, 8.0, ((0, 64),), jnp.float32),
        "up_weight": gaussian(splits[4], (D, FF), D ** -0.5, 0.0625, ((0, 8), (1, 64))),
        "down_weight": gaussian(splits[5], (FF, D), FF ** -0.5, 0.046875, ((0, 64), (1, 8))),
        "mixed_grad": gaussian(splits[6], (SLOTS, D), 1.0, 6.0, ((0, 64), (1, 8))),
    }


def blockwise(left, right):
    blocks = N_VIT * N_SEQ
    width = FF // blocks
    rows_count = left.shape[0]
    left_blocks = left.reshape(rows_count, blocks, width).transpose(1, 0, 2)
    right_blocks = right.reshape(blocks, width, right.shape[1])

    def step(total, pair):
        term = jnp.dot(pair[0], pair[1], preferred_element_type=jnp.float32).astype(jnp.bfloat16)
        term = lax.optimization_barrier(term)
        return total + term.astype(jnp.float32), None

    start = jnp.zeros((rows_count, right.shape[1]), jnp.float32)
    total, unused = lax.scan(step, start, (left_blocks, right_blocks))
    return total


def reference(merged, positions, picked, router_score, up_weight, down_weight, mixed_grad):
    slot_count = N_SEQ * CAP
    group = (jnp.arange(VIS, dtype=jnp.int32) // VIS_GRP).astype(jnp.int32)
    target = (positions // SPAN).astype(jnp.int32)
    owners = jnp.arange(N_SEQ, dtype=jnp.int32)
    onehot = (target[:, None] == owners[None, :]).astype(jnp.int32) * picked[:, None]
    stacked = onehot.reshape(GROUPS, VIS_GRP, N_SEQ)
    ranks = jnp.sum((jnp.cumsum(stacked, axis=1) - stacked) * stacked, axis=2).reshape(VIS).astype(jnp.int32)
    owner = (group // N_SEQ) * N_SEQ + target
    slot = owner * slot_count + (group % N_SEQ) * CAP + ranks
    slot = jnp.where(picked == 1, slot, SLOTS).astype(jnp.int32)
    gate_tok = jax.nn.sigmoid(router_score).astype(jnp.bfloat16)
    rows = jnp.zeros((SLOTS, D), jnp.bfloat16).at[slot].set(merged, mode="drop")
    gates = jnp.zeros((SLOTS,), jnp.bfloat16).at[slot].set(gate_tok, mode="drop")
    pre = jnp.dot(rows, up_weight, preferred_element_type=jnp.float32)
    act = jax.nn.silu(pre).astype(jnp.bfloat16)
    y_rows = blockwise(act, down_weight)
    gates_wide = gates.astype(jnp.float32)[:, None]
    mixed = (rows.astype(jnp.float32) + gates_wide * y_rows).astype(jnp.bfloat16)
    scaled = (gates_wide * mixed_grad.astype(jnp.float32)).astype(jnp.bfloat16)
    down_grad = jnp.dot(act.T, scaled, preferred_element_type=jnp.float32)
    act_grad = jnp.dot(scaled, down_weight.T, preferred_element_type=jnp.float32)
    sig = jax.nn.sigmoid(pre)
    pre_grad = (act_grad * sig * (1.0 + pre * (1.0 - sig))).astype(jnp.bfloat16)
    up_grad = jnp.dot(rows.T, pre_grad, preferred_element_type=jnp.float32)
    row_grad = blockwise(pre_grad, up_weight.T)
    slot_grad = (mixed_grad.astype(jnp.float32) + row_grad).astype(jnp.bfloat16)
    safe = jnp.minimum(slot, SLOTS - 1).astype(jnp.int32)
    token_grad = jnp.where(picked[:, None] == 1, slot_grad[safe], jnp.zeros((), jnp.bfloat16)).astype(jnp.bfloat16)
    return mixed, token_grad, up_grad, down_grad
```

```python
import functools

import jax
import jax.numpy as jnp
from jax import lax
from jax.experimental import pallas as pl
from jax.experimental.pallas import tpu as pltpu
from jax.sharding import PartitionSpec as P

MESH = pl.DeviceIdType.MESH
F32 = jnp.float32
BF16 = jnp.bfloat16
VIT_SEQ = ("vit", "seq")

GROUPS = ((0, 1), (1, 5), (5, 8), (12, 16), (8, 12))
OWN, NEAR_P, FAR_P, NEAR_M, FAR_M = range(5)


def mm(a, b, ca=1, cb=0):
    return lax.dot_general(a, b, (((ca,), (cb,)), ((), ())), preferred_element_type=F32)


def kernel(
    merged, pos, picked, score, cot_in, up_hbm, down_hbm,
    mixed_out, token_out, up_out, down_out,
    up_w, down_w, rows_g, scaled_g, part, part_in, share, share_in, act_g, pg_g,
    terms, y_in, rb, rf, far_p, far_m, fin, relay,
    cot_send, cot_recv, mix_send, mix_recv, up_acc, down_acc,
    local_sem, ag_zrecv, ag_yrecv, ag_send, rs_yrecv, rs_zrecv, rs_send, x_sem, a_sem,
):
    vit, seq, ten = (lax.axis_index(a) for a in ("vit", "seq", "tensor"))
    z = (vit // 4) * 8 + seq
    y = vit % 4
    x, core = ten // 2, ten % 2

    def at_z(k):
        other = (z + k + 16) % 16
        return ((other // 8) * 4 + y, other % 8, ten)

    def at_y(k):
        return ((vit // 4) * 4 + (y + k + 4) % 4, seq, ten)

    def at_ten(k):
        return (vit, seq, (ten + k) % 8)

    def at_x(k):
        return (vit, seq, ((x + k) % 4) * 2 + core)

    partner = (vit, seq, x * 2 + 1 - core)

    def at_seq(k):
        return (vit, (seq + k) % 8, ten)

    def remote(src, dst, send, recv, to):
        return pltpu.make_async_remote_copy(
            src_ref=src, dst_ref=dst, send_sem=send, recv_sem=recv, device_id=to, device_id_type=MESH
        )

    def push(src, dst, send, recv, to):
        remote(src, dst, send, recv, to).start()

    def got(dst, recv):
        remote(dst, dst, recv, recv, partner).wait_recv()

    def sent(src, send):
        remote(src, src, send, send, partner).wait_send()

    load_up = pltpu.make_async_copy(up_hbm, up_w, local_sem.at[0])
    load_down = pltpu.make_async_copy(down_hbm, down_w, local_sem.at[1])
    load_up.start()
    load_down.start()

    barrier = pltpu.get_barrier_semaphore()
    peers = [at_z(k) for k in (4, -4, 3, -3, 2, -2, 1, -1)]
    peers += [at_y(1), at_y(-1)]
    peers += [at_ten(k) for k in range(1, 8)]
    peers += [at_seq(k) for k in range(1, 8)]
    for peer in peers:
        pl.semaphore_signal(barrier, inc=1, device_id=peer, device_id_type=MESH)

    n = pos.shape[1]
    t_row = (pos[...] >> 14).astype(F32)
    p_row = picked[...].astype(F32)
    i0 = lax.broadcasted_iota(jnp.int32, (n, n), 0)
    i1 = lax.broadcasted_iota(jnp.int32, (n, n), 1)
    eye = i0 == i1
    t_wide = jnp.broadcast_to(t_row, (n, n))
    p_wide = jnp.broadcast_to(p_row, (n, n))
    t_col = jnp.sum(jnp.where(eye, t_wide, 0.0), axis=1, keepdims=True)
    p_col = jnp.sum(jnp.where(eye, p_wide, 0.0), axis=1, keepdims=True)
    same = t_col == t_wide
    c_row = jnp.sum(jnp.where(i0 < i1, p_col, 0.0), axis=0, keepdims=True)
    c_col = jnp.sum(jnp.where(i1 < i0, p_wide, 0.0), axis=1, keepdims=True)
    rank_row = jnp.sum(jnp.where((i0 < i1) & same, p_col, 0.0), axis=0, keepdims=True)
    rank_col = jnp.sum(jnp.where((i1 < i0) & same, p_wide, 0.0), axis=1, keepdims=True)
    slot_row = t_row * 2.0 + rank_row
    slot_col = t_col * 2.0 + rank_col

    def hot(values, on, shape, dim):
        ids = lax.broadcasted_iota(jnp.int32, shape, dim).astype(F32)
        return jnp.where(values == ids, on, 0.0)

    pick_f = hot(c_row, p_row, (8, n), 0)
    pick = pick_f.astype(BF16)
    pick_t = hot(c_col, p_col, (n, 8), 1).astype(BF16)
    slots = hot(slot_row, p_row, (16, n), 0).astype(BF16)
    slots_t = hot(slot_col, p_col, (n, 16), 1).astype(BF16)
    place = mm(slots, pick_t).astype(BF16)
    place_t = mm(pick, slots_t).astype(BF16)
    gate_tok = jax.nn.sigmoid(score[...]).astype(BF16).astype(F32)
    gate = jnp.sum(pick_f * gate_tok, axis=1, keepdims=True)
    rows_g[0, 0] = mm(pick, merged[...]).astype(BF16)
    cot_send[...] = cot_in[...].reshape(8, 2, cot_in.shape[1])

    pl.semaphore_wait(barrier, len(peers))

    def gather(k, buf):
        send_z, send_y = ag_send.at[k, 0], ag_send.at[k, 1]

        def z_one(slot, back, dist):
            push(buf.at[0, slot], buf.at[0, back], send_z, ag_zrecv.at[k, back], at_z(dist))

        def first():
            for d in (4, 3, 2, 1):
                z_one(0, 16 - d, d)
                z_one(0, d, -d)

        def second():
            got(buf.at[0, 12], ag_zrecv.at[k, 12])
            for d in (4, 3, 2, 1):
                z_one(12, 12 - d, d)
            got(buf.at[0, 4], ag_zrecv.at[k, 4])
            for d in (3, 2, 1):
                z_one(4, 4 + d, -d)

        def spread(g):
            lo, hi = GROUPS[g]
            for s in range(lo, hi):
                if s not in (0, 4, 12):
                    got(buf.at[0, s], ag_zrecv.at[k, s])
            r = pl.ds(lo, hi - lo)
            push(buf.at[0, r], buf.at[3, r], send_y, ag_yrecv.at[k, 3, g], at_y(1))
            push(buf.at[0, r], buf.at[1, r], send_y, ag_yrecv.at[k, 1, g], at_y(-1))

        def relay_on(g):
            lo, hi = GROUPS[g]
            r = pl.ds(lo, hi - lo)
            q, to = (1, -1) if g in (NEAR_M, FAR_M) else (3, 1)
            got(buf.at[q, r], ag_yrecv.at[k, q, g])
            push(buf.at[q, r], buf.at[2, r], send_y, ag_yrecv.at[k, 2, g], at_y(to))

        def finish():
            for g, (lo, hi) in enumerate(GROUPS):
                r = pl.ds(lo, hi - lo)
                q = 3 if g in (NEAR_M, FAR_M) else 1
                got(buf.at[q, r], ag_yrecv.at[k, q, g])
                got(buf.at[2, r], ag_yrecv.at[k, 2, g])

        def drain():
            sent(buf.at[0, pl.ds(0, 15)], send_z)
            sent(buf.at[pl.ds(0, 3)], send_y)

        return first, second, spread, relay_on, finish, drain

    def hidden_sum(k):
        def exchange(value):
            part[k] = value.reshape(part.shape[1:])
            push(part.at[k, 1 - core], part_in.at[k], x_sem.at[k, 0], x_sem.at[k, 1], partner)

        def scatter():
            got(part_in.at[k], x_sem.at[k, 1])
            share[k] = part[k, core] + part_in[k]
            for j in (2, 1, 3):
                push(
                    share.at[k, (x + j) % 4], share_in.at[k, j - 1],
                    x_sem.at[k, 2], x_sem.at[k, 3], at_x(j),
                )

        def total():
            got(share_in.at[k], x_sem.at[k, 3])
            return share[k, x] + share_in[k, 0] + share_in[k, 1] + share_in[k, 2]

        def widen(buf, value):
            buf[core * 4 + x] = value.astype(BF16)
            mine = buf.at[core * 4 + x]
            for j in (4, 5, 2, 3, 6, 7, 1):
                push(mine, mine, x_sem.at[k, 4], x_sem.at[k, 5], at_ten(j))

        def widened(buf):
            got(buf.at[pl.ds(0, 7)], x_sem.at[k, 5])
            return buf[...].reshape(-1, buf.shape[-1])

        def drain():
            sent(part_in.at[k], x_sem.at[k, 0])
            sent(share_in.at[k], x_sem.at[k, 2])
            sent(act_g.at[pl.ds(0, 7)], x_sem.at[k, 4])

        return exchange, scatter, total, widen, widened, drain

    def reduce_rows(k):
        t, yi, r16 = terms.at[k], y_in.at[k], rb.at[k]
        send_y, send_z = rs_send.at[k, 0], rs_send.at[k, 1]
        plus, minus = {0: (5, 8), 1: (0, 5)}, {0: (8, 12), 1: (12, 16)}

        def y_push(kind, q, lo, hi, to, f):
            r = pl.ds(lo, hi - lo)
            s = pl.ds(lo % 8, hi - lo)
            push(t.at[q, r], yi.at[kind, s], send_y, rs_yrecv.at[k, kind, f], at_y(to))

        def y_got(kind, lo, hi, f):
            got(yi.at[kind, pl.ds(lo % 8, hi - lo)], rs_yrecv.at[k, kind, f])

        def start(value):
            terms[k] = value.astype(BF16).reshape(terms.shape[1:])
            for f in (0, 1):
                y_push(0, 2, *plus[f], 1, f)
                y_push(1, 2, *minus[f], -1, f)
                y_push(2, 3, *plus[f], -1, f)
                y_push(3, 1, *minus[f], 1, f)

        def add(q, lo, hi, kind):
            return t[q, lo:hi].astype(F32) + yi[kind, lo % 8 : lo % 8 + hi - lo].astype(F32)

        def y_second(f):
            lo, hi = plus[f]
            y_got(0, lo, hi, f)
            t[1, lo:hi] = add(1, lo, hi, 0).astype(BF16)
            y_push(4, 1, lo, hi, 1, f)
            lo, hi = minus[f]
            y_got(1, lo, hi, f)
            t[3, lo:hi] = add(3, lo, hi, 1).astype(BF16)
            y_push(5, 3, lo, hi, -1, f)

        def y_end(f):
            for kinds, (lo, hi) in (((2, 4), plus[f]), ((3, 5), minus[f])):
                for kind in kinds:
                    y_got(kind, lo, hi, f)
                both = add(0, lo, hi, kinds[0]) + yi[kinds[1], lo % 8 : lo % 8 + hi - lo].astype(F32)
                rf[k, lo:hi] = both
                rb[k, lo:hi] = both.astype(BF16)

        def z_far():
            y_end(0)
            for d in (4, 3, 2, 1):
                push(r16.at[4 + d], far_p.at[k, d - 1], send_z, rs_zrecv.at[k, 0], at_z(d))
            for d in (3, 2, 1):
                push(r16.at[12 - d], far_m.at[k, d - 1], send_z, rs_zrecv.at[k, 1], at_z(-d))

        def z_near():
            y_end(1)
            for d in (3, 2, 1):
                push(r16.at[d], fin.at[k, d - 1], send_z, rs_zrecv.at[k, 2], at_z(d))
                push(r16.at[16 - d], fin.at[k, d + 2], send_z, rs_zrecv.at[k, 2], at_z(-d))

        def z_relay():
            got(far_p.at[k], rs_zrecv.at[k, 0])
            total = rf[k, 4]
            for d in range(4):
                total += far_p[k, d].astype(F32)
            relay[k, 0] = total.astype(BF16)
            push(relay.at[k, 0], fin.at[k, 6], send_z, rs_zrecv.at[k, 2], at_z(4))
            got(far_m.at[k], rs_zrecv.at[k, 1])
            total = rf[k, 12]
            for d in range(3):
                total += far_m[k, d].astype(F32)
            relay[k, 1] = total.astype(BF16)
            push(relay.at[k, 1], fin.at[k, 7], send_z, rs_zrecv.at[k, 2], at_z(-4))

        def result():
            got(fin.at[k], rs_zrecv.at[k, 2])
            total = rf[k, 0]
            for d in range(8):
                total += fin[k, d].astype(F32)
            return total

        def drain():
            sent(t.at[pl.ds(0, 3)], send_y)
            sent(r16.at[pl.ds(0, 15)], send_z)

        return start, y_second, z_far, z_near, z_relay, result, drain

    def seq_send(k, src, dst):
        for j in (7, 6, 5, 4, 3, 2, 1):
            push(src.at[(seq + j) % 8], dst.at[seq], a_sem.at[k, 0], a_sem.at[k, 1], at_seq(j))
        dst[seq] = src[seq]

    def seq_got(k, dst):
        got(dst.at[pl.ds(0, 7)], a_sem.at[k, 1])
        return dst[...].reshape(16, dst.shape[-1])

    r_first, r_second, r_spread, r_relay, r_finish, r_drain = gather(0, rows_g)
    s_first, s_second, s_spread, s_relay, s_finish, s_drain = gather(1, scaled_g)
    h0 = hidden_sum(0)
    h1 = hidden_sum(1)
    y0 = reduce_rows(0)
    y1 = reduce_rows(1)

    r_first()
    seq_send(0, cot_send, cot_recv)
    r_spread(OWN)
    r_second()
    r_spread(NEAR_P)
    r_spread(NEAR_M)
    r_relay(OWN)
    cot = mm(place_t, seq_got(0, cot_recv))
    scaled_g[0, 0] = (gate * cot).astype(BF16)
    s_first()
    s_spread(OWN)
    r_relay(NEAR_P)
    r_relay(NEAR_M)
    r_spread(FAR_M)
    r_spread(FAR_P)
    s_second()
    r_relay(FAR_M)
    r_relay(FAR_P)
    s_relay(OWN)
    s_spread(NEAR_P)
    s_spread(NEAR_M)
    r_finish()
    load_up.wait()
    every_row = rows_g[...].reshape(512, -1)
    h0[0](mm(every_row, up_w[...]))
    s_spread(FAR_M)
    s_spread(FAR_P)
    s_relay(NEAR_P)
    s_relay(NEAR_M)
    h0[1]()
    s_relay(FAR_M)
    s_relay(FAR_P)
    pre = h0[2]()
    sig = jax.nn.sigmoid(pre)
    h0[3](act_g, pre * sig)
    s_finish()
    load_down.wait()
    every_scaled = scaled_g[...].reshape(512, -1)
    h1[0](mm(every_scaled, down_w[...], 1, 1))
    act = h0[4](act_g)
    y0[0](mm(act, down_w[...]))
    h1[1]()
    y0[1](0)
    act_grad = h1[2]()
    h1[3](pg_g, act_grad * sig * (1.0 + pre * (1.0 - sig)))
    y0[1](1)
    y0[2]()
    pre_grad = h1[4](pg_g)
    y1[0](mm(pre_grad, up_w[...], 1, 1))
    y0[3]()
    down_acc[...] = mm(act, every_scaled, 0, 0)
    store_down = pltpu.make_async_copy(down_acc, down_out, local_sem.at[2])
    store_down.start()
    y0[4]()
    y1[1](0)
    y1[1](1)
    y1[2]()
    up_acc[...] = mm(every_row, pre_grad, 0, 0)
    store_up = pltpu.make_async_copy(up_acc, up_out, local_sem.at[3])
    store_up.start()
    mixed = (rows_g[0, 0].astype(F32) + gate * y0[5]()).astype(BF16)
    mix_send[...] = mm(place, mixed).astype(BF16).reshape(mix_send.shape)
    seq_send(1, mix_send, mix_recv)
    y1[3]()
    y1[4]()
    slot_grad = (cot + y1[5]()).astype(BF16)
    token_out[...] = mm(pick_t, slot_grad).astype(BF16)
    mixed_out[...] = seq_got(1, mix_recv)

    store_down.wait()
    store_up.wait()
    r_drain()
    s_drain()
    h0[5]()
    h1[5]()
    y0[6]()
    y1[6]()
    sent(cot_recv.at[pl.ds(0, 7)], a_sem.at[0, 0])
    sent(mix_recv.at[pl.ds(0, 7)], a_sem.at[1, 0])


def per_device(merged, positions, picked, router_score, up_weight, down_weight, mixed_grad):
    width = merged.shape[1]
    hidden = up_weight.shape[1]
    vmem = pl.BlockSpec(memory_space=pltpu.VMEM)
    hbm = pl.BlockSpec(memory_space=pl.ANY)
    dma = pltpu.SemaphoreType.DMA
    block = (8, width)
    return pl.pallas_call(
        kernel,
        name="routed_ffn",
        out_shape=(
            jax.ShapeDtypeStruct(mixed_grad.shape, BF16),
            jax.ShapeDtypeStruct(merged.shape, BF16),
            jax.ShapeDtypeStruct(up_weight.shape, F32),
            jax.ShapeDtypeStruct(down_weight.shape, F32),
        ),
        in_specs=[vmem] * 5 + [hbm] * 2,
        out_specs=(vmem, vmem, hbm, hbm),
        scratch_shapes=[
            pltpu.VMEM(up_weight.shape, BF16),
            pltpu.VMEM(down_weight.shape, BF16),
            pltpu.VMEM((4, 16, *block), BF16),
            pltpu.VMEM((4, 16, *block), BF16),
            pltpu.VMEM((2, 2, 4, 64, hidden), F32),
            pltpu.VMEM((2, 4, 64, hidden), F32),
            pltpu.VMEM((2, 4, 64, hidden), F32),
            pltpu.VMEM((2, 3, 64, hidden), F32),
            pltpu.VMEM((8, 64, hidden), BF16),
            pltpu.VMEM((8, 64, hidden), BF16),
            pltpu.VMEM((2, 4, 16, *block), BF16),
            pltpu.VMEM((2, 6, 8, *block), BF16),
            pltpu.VMEM((2, 16, *block), BF16),
            pltpu.VMEM((2, 16, *block), F32),
            pltpu.VMEM((2, 4, *block), BF16),
            pltpu.VMEM((2, 3, *block), BF16),
            pltpu.VMEM((2, 8, *block), BF16),
            pltpu.VMEM((2, 2, *block), BF16),
            pltpu.VMEM((8, 2, width), BF16),
            pltpu.VMEM((8, 2, width), BF16),
            pltpu.VMEM((8, 2, width), BF16),
            pltpu.VMEM((8, 2, width), BF16),
            pltpu.VMEM(up_weight.shape, F32),
            pltpu.VMEM(down_weight.shape, F32),
            dma((4,)),
            dma((2, 16)),
            dma((2, 4, 5)),
            dma((2, 2)),
            dma((2, 6, 2)),
            dma((2, 3)),
            dma((2, 2)),
            dma((2, 6)),
            dma((2, 2)),
        ],
        compiler_params=pltpu.CompilerParams(
            collective_id=0, has_side_effects=True, vmem_limit_bytes=48 * 1024 * 1024
        ),
    )(
        merged,
        positions.reshape(1, -1),
        picked.reshape(1, -1),
        router_score.reshape(1, -1),
        mixed_grad,
        up_weight,
        down_weight,
    )


def solution(mesh):
    placed = (
        P(VIT_SEQ, "tensor"),
        P(VIT_SEQ),
        P(VIT_SEQ),
        P(VIT_SEQ),
        P("tensor", VIT_SEQ),
        P(VIT_SEQ, "tensor"),
        P(VIT_SEQ, "tensor"),
    )
    return jax.shard_map(
        per_device,
        mesh=mesh,
        in_specs=placed,
        out_specs=(
            P(VIT_SEQ, "tensor"),
            P(VIT_SEQ, "tensor"),
            P("tensor", VIT_SEQ),
            P(VIT_SEQ, "tensor"),
        ),
        check_vma=False,
    )
```

```python
import functools

import jax
import jax.numpy as jnp
from jax import lax
from jax.experimental import pallas as pl
from jax.experimental.pallas import tpu as pltpu
from jax.sharding import PartitionSpec as P

MESH = pl.DeviceIdType.MESH
F32 = jnp.float32
BF16 = jnp.bfloat16
VIT_SEQ = ("vit", "seq")

GROUPS = ((0, 1), (1, 5), (5, 8), (12, 16), (8, 12))
OWN, NEAR_P, FAR_P, NEAR_M, FAR_M = range(5)


def mm(a, b, ca=1, cb=0):
    return lax.dot_general(a, b, (((ca,), (cb,)), ((), ())), preferred_element_type=F32)


def kernel(
    merged_hbm, pos_hbm, picked_hbm, score_hbm, cot_hbm, up_hbm, down_hbm,
    mixed_hbm, token_hbm, up_grad_hbm, down_grad_hbm,
    merged, pos, picked, score, cot_in, up_w, down_w, rows_g, scaled_g, part, part_in, share, share_in, act_g, pg_g,
    terms, y_in, rb, rf, far_p, far_m, fin, relay,
    cot_send, cot_recv, mix_send, mix_recv, share_f,
    mixed_out, token_out, up_out, down_out,
    local_sem, ag_zrecv, ag_yrecv, ag_send, rs_yrecv, rs_zrecv, rs_send, x_sem, a_sem,
):
    vit, seq, ten = (lax.axis_index(a) for a in ("vit", "seq", "tensor"))
    z = (vit // 4) * 8 + seq
    y = vit % 4
    x, core = ten // 2, ten % 2

    def at_z(k):
        other = (z + k + 16) % 16
        return ((other // 8) * 4 + y, other % 8, ten)

    def at_y(k):
        return ((vit // 4) * 4 + (y + k + 4) % 4, seq, ten)

    def at_ten(k):
        return (vit, seq, (ten + k) % 8)

    def at_x(k):
        return (vit, seq, ((x + k) % 4) * 2 + core)

    partner = (vit, seq, x * 2 + 1 - core)

    def at_seq(k):
        return (vit, (seq + k) % 8, ten)

    def remote(src, dst, send, recv, to):
        return pltpu.make_async_remote_copy(
            src_ref=src, dst_ref=dst, send_sem=send, recv_sem=recv, device_id=to, device_id_type=MESH
        )

    def push(src, dst, send, recv, to):
        remote(src, dst, send, recv, to).start()

    def got(dst, recv):
        remote(dst, dst, recv, recv, partner).wait_recv()

    def sent(src, send):
        remote(src, src, send, send, partner).wait_send()

    loads = [
        pltpu.make_async_copy(src, dst, local_sem.at[i])
        for i, (src, dst) in enumerate(
            (
                (pos_hbm, pos), (picked_hbm, picked), (merged_hbm, merged), (cot_hbm, cot_in),
                (score_hbm, score), (up_hbm, up_w), (down_hbm, down_w),
            )
        )
    ]
    for load in loads:
        load.start()

    stores = [
        pltpu.make_async_copy(src, dst, local_sem.at[7 + i])
        for i, (src, dst) in enumerate(
            (
                (mixed_out, mixed_hbm), (token_out, token_hbm),
                (up_out, up_grad_hbm), (down_out, down_grad_hbm),
            )
        )
    ]

    barrier = pltpu.get_barrier_semaphore()
    peers = [at_z(k) for k in (4, -4, 3, -3, 2, -2, 1, -1)]
    peers += [at_y(1), at_y(-1)]
    peers += [at_ten(k) for k in range(1, 8)]
    peers += [at_seq(k) for k in range(1, 8)]
    for peer in peers:
        pl.semaphore_signal(barrier, inc=1, device_id=peer, device_id_type=MESH)

    n = pos.shape[1]
    i0 = lax.broadcasted_iota(jnp.int32, (n, n), 0)
    i1 = lax.broadcasted_iota(jnp.int32, (n, n), 1)
    eye = i0 == i1

    def hot(values, on, shape, dim):
        ids = lax.broadcasted_iota(jnp.int32, shape, dim).astype(F32)
        return jnp.where(values == ids, on, 0.0)

    loads[1].wait()
    p_row = picked[...].astype(F32)
    p_wide = jnp.broadcast_to(p_row, (n, n))
    p_col = jnp.sum(jnp.where(eye, p_wide, 0.0), axis=1, keepdims=True)
    c_row = jnp.sum(jnp.where(i0 < i1, p_col, 0.0), axis=0, keepdims=True)
    pick_f = hot(c_row, p_row, (8, n), 0)
    pick = pick_f.astype(BF16)
    loads[2].wait()
    rows_g[0, 0] = mm(pick, merged[...]).astype(BF16)
    loads[3].wait()
    cot_send[...] = cot_in[...].reshape(8, 2, cot_in.shape[1])

    pl.semaphore_wait(barrier, len(peers))

    def routing():
        loads[0].wait()
        t_row = (pos[...] >> 14).astype(F32)
        t_wide = jnp.broadcast_to(t_row, (n, n))
        t_col = jnp.sum(jnp.where(eye, t_wide, 0.0), axis=1, keepdims=True)
        same = t_col == t_wide
        c_col = jnp.sum(jnp.where(i1 < i0, p_wide, 0.0), axis=1, keepdims=True)
        rank_row = jnp.sum(jnp.where((i0 < i1) & same, p_col, 0.0), axis=0, keepdims=True)
        rank_col = jnp.sum(jnp.where((i1 < i0) & same, p_wide, 0.0), axis=1, keepdims=True)
        slot_row = t_row * 2.0 + rank_row
        slot_col = t_col * 2.0 + rank_col
        pick_t = hot(c_col, p_col, (n, 8), 1).astype(BF16)
        slots = hot(slot_row, p_row, (16, n), 0).astype(BF16)
        slots_t = hot(slot_col, p_col, (n, 16), 1).astype(BF16)
        place = mm(slots, pick_t).astype(BF16)
        place_t = mm(pick, slots_t).astype(BF16)
        loads[4].wait()
        gate_tok = jax.nn.sigmoid(score[...]).astype(BF16).astype(F32)
        gate = jnp.sum(pick_f * gate_tok, axis=1, keepdims=True)
        return pick_t, place, place_t, gate

    def gather(k, buf):
        send_z, send_y = ag_send.at[k, 0], ag_send.at[k, 1]

        def z_one(slot, back, dist):
            push(buf.at[0, slot], buf.at[0, back], send_z, ag_zrecv.at[k, back], at_z(dist))

        def first():
            for d in (4, 3, 2, 1):
                z_one(0, 16 - d, d)
                z_one(0, d, -d)

        def second():
            got(buf.at[0, 12], ag_zrecv.at[k, 12])
            for d in (4, 3, 2, 1):
                z_one(12, 12 - d, d)
            got(buf.at[0, 4], ag_zrecv.at[k, 4])
            for d in (3, 2, 1):
                z_one(4, 4 + d, -d)

        def spread(g):
            lo, hi = GROUPS[g]
            for s in range(lo, hi):
                if s not in (0, 4, 12):
                    got(buf.at[0, s], ag_zrecv.at[k, s])
            r = pl.ds(lo, hi - lo)
            push(buf.at[0, r], buf.at[3, r], send_y, ag_yrecv.at[k, 3, g], at_y(1))
            push(buf.at[0, r], buf.at[1, r], send_y, ag_yrecv.at[k, 1, g], at_y(-1))

        def relay_on(g):
            lo, hi = GROUPS[g]
            r = pl.ds(lo, hi - lo)
            q, to = (1, -1) if g in (NEAR_M, FAR_M) else (3, 1)
            got(buf.at[q, r], ag_yrecv.at[k, q, g])
            push(buf.at[q, r], buf.at[2, r], send_y, ag_yrecv.at[k, 2, g], at_y(to))

        def finish():
            for g, (lo, hi) in enumerate(GROUPS):
                r = pl.ds(lo, hi - lo)
                q = 3 if g in (NEAR_M, FAR_M) else 1
                got(buf.at[q, r], ag_yrecv.at[k, q, g])
                got(buf.at[2, r], ag_yrecv.at[k, 2, g])

        def drain():
            sent(buf.at[0, pl.ds(0, 15)], send_z)
            sent(buf.at[pl.ds(0, 3)], send_y)

        return first, second, spread, relay_on, finish, drain

    def hidden_sum(k):
        def exchange(value):
            part[k] = value.reshape(part.shape[1:])
            push(part.at[k, 1 - core], part_in.at[k], x_sem.at[k, 0], x_sem.at[k, 1], partner)

        def scatter():
            got(part_in.at[k], x_sem.at[k, 1])
            both = part[k, core] + part_in[k]
            share_f[k] = both
            share[k] = both.astype(BF16)
            for j in (2, 1, 3):
                push(
                    share.at[k, (x + j) % 4], share_in.at[k, j - 1],
                    x_sem.at[k, 2], x_sem.at[k, 3], at_x(j),
                )

        def total():
            got(share_in.at[k], x_sem.at[k, 3])
            arrived = share_in[k].astype(F32)
            return share_f[k, x] + arrived[0] + arrived[1] + arrived[2]

        def widen(buf, value):
            buf[core * 4 + x] = value.astype(BF16)
            mine = buf.at[core * 4 + x]
            for j in (2, 1, 3):
                push(mine, mine, x_sem.at[k, 4], x_sem.at[k, 5], at_x(j))

        def pair(buf):
            got(buf.at[pl.ds(0, 3)], x_sem.at[k, 5])
            half = buf.at[pl.ds(core * 4, 4)]
            push(half, half, x_sem.at[k, 6], x_sem.at[k, 7], partner)

        def widened(buf):
            got(buf.at[pl.ds(0, 4)], x_sem.at[k, 7])
            return buf[...].reshape(-1, buf.shape[-1])

        def drain():
            sent(part_in.at[k], x_sem.at[k, 0])
            sent(share_in.at[k], x_sem.at[k, 2])
            sent(act_g.at[pl.ds(0, 3)], x_sem.at[k, 4])
            sent(act_g.at[pl.ds(0, 4)], x_sem.at[k, 6])

        return exchange, scatter, total, widen, pair, widened, drain

    def reduce_rows(k):
        t, yi, r16 = terms.at[k], y_in.at[k], rb.at[k]
        send_y, send_z = rs_send.at[k, 0], rs_send.at[k, 1]
        plus, minus = {0: (5, 8), 1: (0, 5)}, {0: (8, 12), 1: (12, 16)}

        def y_push(kind, q, lo, hi, to, f):
            r = pl.ds(lo, hi - lo)
            s = pl.ds(lo % 8, hi - lo)
            push(t.at[q, r], yi.at[kind, s], send_y, rs_yrecv.at[k, kind, f], at_y(to))

        def y_got(kind, lo, hi, f):
            got(yi.at[kind, pl.ds(lo % 8, hi - lo)], rs_yrecv.at[k, kind, f])

        def start(value):
            terms[k] = value.astype(BF16).reshape(terms.shape[1:])
            for f in (0, 1):
                y_push(0, 2, *plus[f], 1, f)
                y_push(1, 2, *minus[f], -1, f)
                if f == 0:
                    y_push(2, 3, *plus[f], -1, f)
                    y_push(3, 1, *minus[f], 1, f)

        def start_near():
            y_push(2, 3, *plus[1], -1, 1)
            y_push(3, 1, *minus[1], 1, 1)

        def add(q, lo, hi, kind):
            return t[q, lo:hi].astype(F32) + yi[kind, lo % 8 : lo % 8 + hi - lo].astype(F32)

        def y_second(f):
            lo, hi = plus[f]
            y_got(0, lo, hi, f)
            t[1, lo:hi] = add(1, lo, hi, 0).astype(BF16)
            y_push(4, 1, lo, hi, 1, f)
            lo, hi = minus[f]
            y_got(1, lo, hi, f)
            t[3, lo:hi] = add(3, lo, hi, 1).astype(BF16)
            y_push(5, 3, lo, hi, -1, f)

        def y_end(f):
            for kinds, (lo, hi) in (((2, 4), plus[f]), ((3, 5), minus[f])):
                for kind in kinds:
                    y_got(kind, lo, hi, f)
                both = add(0, lo, hi, kinds[0]) + yi[kinds[1], lo % 8 : lo % 8 + hi - lo].astype(F32)
                rf[k, lo:hi] = both
                rb[k, lo:hi] = both.astype(BF16)

        def z_far():
            y_end(0)
            for d in (4, 3, 2, 1):
                push(r16.at[4 + d], far_p.at[k, d - 1], send_z, rs_zrecv.at[k, 0], at_z(d))
            for d in (3, 2, 1):
                push(r16.at[12 - d], far_m.at[k, d - 1], send_z, rs_zrecv.at[k, 1], at_z(-d))

        def z_near():
            y_end(1)
            for d in (3, 2, 1):
                push(r16.at[d], fin.at[k, d - 1], send_z, rs_zrecv.at[k, 2], at_z(d))
                push(r16.at[16 - d], fin.at[k, d + 2], send_z, rs_zrecv.at[k, 2], at_z(-d))

        def z_relay():
            got(far_p.at[k], rs_zrecv.at[k, 0])
            total = rf[k, 4]
            for d in range(4):
                total += far_p[k, d].astype(F32)
            relay[k, 0] = total.astype(BF16)
            push(relay.at[k, 0], fin.at[k, 6], send_z, rs_zrecv.at[k, 2], at_z(4))
            got(far_m.at[k], rs_zrecv.at[k, 1])
            total = rf[k, 12]
            for d in range(3):
                total += far_m[k, d].astype(F32)
            relay[k, 1] = total.astype(BF16)
            push(relay.at[k, 1], fin.at[k, 7], send_z, rs_zrecv.at[k, 2], at_z(-4))

        def result():
            got(fin.at[k], rs_zrecv.at[k, 2])
            total = rf[k, 0]
            for d in range(8):
                total += fin[k, d].astype(F32)
            return total

        def drain():
            sent(t.at[pl.ds(0, 3)], send_y)
            sent(r16.at[pl.ds(0, 15)], send_z)

        return start, start_near, y_second, z_far, z_near, z_relay, result, drain

    def seq_send(k, src, dst):
        for j in (7, 6, 5, 4, 3, 2, 1):
            push(src.at[(seq + j) % 8], dst.at[seq], a_sem.at[k, 0], a_sem.at[k, 1], at_seq(j))
        dst[seq] = src[seq]

    def seq_got(k, dst):
        got(dst.at[pl.ds(0, 7)], a_sem.at[k, 1])
        return dst[...].reshape(16, dst.shape[-1])

    r_first, r_second, r_spread, r_relay, r_finish, r_drain = gather(0, rows_g)
    s_first, s_second, s_spread, s_relay, s_finish, s_drain = gather(1, scaled_g)
    h0 = hidden_sum(0)
    h1 = hidden_sum(1)
    y0 = reduce_rows(0)
    y1 = reduce_rows(1)

    h0_exchange, h0_scatter, h0_total, h0_widen, h0_pair, h0_widened, h0_drain = h0
    h1_exchange, h1_scatter, h1_total, h1_widen, h1_pair, h1_widened, h1_drain = h1
    y0_start, y0_near, y0_second, y0_z_far, y0_z_near, y0_z_relay, y0_result, y0_drain = y0
    y1_start, y1_near, y1_second, y1_z_far, y1_z_near, y1_z_relay, y1_result, y1_drain = y1

    seq_send(0, cot_send, cot_recv)
    r_first()
    r_spread(OWN)
    pick_t, place, place_t, gate = routing()
    r_second()
    r_spread(NEAR_P)
    r_spread(NEAR_M)
    cot = mm(place_t, seq_got(0, cot_recv))
    scaled_g[0, 0] = (gate * cot).astype(BF16)
    s_first()
    s_spread(OWN)
    r_relay(OWN)
    r_relay(NEAR_P)
    r_relay(NEAR_M)
    r_spread(FAR_M)
    r_spread(FAR_P)
    s_second()
    s_relay(OWN)
    r_relay(FAR_M)
    r_relay(FAR_P)
    s_spread(NEAR_P)
    s_spread(NEAR_M)
    r_finish()
    loads[5].wait()
    every_row = rows_g[...].reshape(512, -1)
    h0_exchange(mm(every_row, up_w[...]))
    s_spread(FAR_M)
    s_spread(FAR_P)
    s_relay(NEAR_P)
    s_relay(NEAR_M)
    h0_scatter()
    s_relay(FAR_M)
    s_relay(FAR_P)
    pre = h0_total()
    sig = jax.nn.sigmoid(pre)
    h0_widen(act_g, pre * sig)
    s_finish()
    loads[6].wait()
    every_scaled = scaled_g[...].reshape(512, -1)
    h1_exchange(mm(every_scaled, down_w[...], 1, 1))
    h0_pair(act_g)
    h1_scatter()
    act = h0_widened(act_g)
    y0_start(mm(act, down_w[...]))
    act_grad = h1_total()
    h1_widen(pg_g, act_grad * sig * (1.0 + pre * (1.0 - sig)))
    y0_second(0)
    y0_near()
    h1_pair(pg_g)
    y0_second(1)
    y0_z_far()
    pre_grad = h1_widened(pg_g)
    y1_start(mm(pre_grad, up_w[...], 1, 1))
    y0_z_near()
    down_out[...] = mm(act, every_scaled, 0, 0)
    stores[3].start()
    y1_second(0)
    y1_near()
    y0_z_relay()
    y1_second(1)
    y1_z_far()
    up_out[...] = mm(every_row, pre_grad, 0, 0)
    stores[2].start()
    y1_z_near()
    mixed = (rows_g[0, 0].astype(F32) + gate * y0_result()).astype(BF16)
    mix_send[...] = mm(place, mixed).astype(BF16).reshape(mix_send.shape)
    seq_send(1, mix_send, mix_recv)
    y1_z_relay()
    slot_grad = (cot + y1_result()).astype(BF16)
    token_out[...] = mm(pick_t, slot_grad).astype(BF16)
    stores[1].start()
    mixed_out[...] = seq_got(1, mix_recv)
    stores[0].start()

    r_drain()
    s_drain()
    h0_drain()
    h1_drain()
    y0_drain()
    y1_drain()
    sent(cot_recv.at[pl.ds(0, 7)], a_sem.at[0, 0])
    sent(mix_recv.at[pl.ds(0, 7)], a_sem.at[1, 0])
    for store in stores:
        store.wait()


def put_out(*refs):
    ins, outs, bufs, sem = refs[:4], refs[4:8], refs[8:12], refs[12]
    pieces = []
    for i, count in ((2, 4), (3, 4), (0, 1), (1, 1)):
        rows = ins[i].shape[0] // count
        for j in range(count):
            part = pl.ds(j * rows, rows)
            n = len(pieces)
            pieces.append(
                (
                    pltpu.make_async_copy(ins[i].at[part], bufs[i].at[part], sem.at[0, n]),
                    pltpu.make_async_copy(bufs[i].at[part], outs[i].at[part], sem.at[1, n]),
                )
            )
    for taken, _ in pieces:
        taken.start()
    for taken, put in pieces:
        taken.wait()
        put.start()
    for _, put in pieces:
        put.wait()


def per_device(merged, positions, picked, router_score, up_weight, down_weight, mixed_grad):
    width = merged.shape[1]
    hidden = up_weight.shape[1]
    hbm = pl.BlockSpec(memory_space=pltpu.HBM)
    dma = pltpu.SemaphoreType.DMA
    block = (8, width)
    results = pl.pallas_call(
        kernel,
        name="routed_ffn",
        out_shape=(
            jax.ShapeDtypeStruct(mixed_grad.shape, BF16),
            jax.ShapeDtypeStruct(merged.shape, BF16),
            jax.ShapeDtypeStruct(up_weight.shape, F32),
            jax.ShapeDtypeStruct(down_weight.shape, F32),
        ),
        in_specs=[hbm] * 7,
        out_specs=(hbm,) * 4,
        scratch_shapes=[
            pltpu.VMEM(merged.shape, BF16),
            pltpu.VMEM((1, merged.shape[0]), jnp.int32),
            pltpu.VMEM((1, merged.shape[0]), jnp.int32),
            pltpu.VMEM((1, merged.shape[0]), F32),
            pltpu.VMEM(mixed_grad.shape, BF16),
            pltpu.VMEM(up_weight.shape, BF16),
            pltpu.VMEM(down_weight.shape, BF16),
            pltpu.VMEM((4, 16, *block), BF16),
            pltpu.VMEM((4, 16, *block), BF16),
            pltpu.VMEM((2, 2, 4, 64, hidden), F32),
            pltpu.VMEM((2, 4, 64, hidden), F32),
            pltpu.VMEM((2, 4, 64, hidden), BF16),
            pltpu.VMEM((2, 3, 64, hidden), BF16),
            pltpu.VMEM((8, 64, hidden), BF16),
            pltpu.VMEM((8, 64, hidden), BF16),
            pltpu.VMEM((2, 4, 16, *block), BF16),
            pltpu.VMEM((2, 6, 8, *block), BF16),
            pltpu.VMEM((2, 16, *block), BF16),
            pltpu.VMEM((2, 16, *block), F32),
            pltpu.VMEM((2, 4, *block), BF16),
            pltpu.VMEM((2, 3, *block), BF16),
            pltpu.VMEM((2, 8, *block), BF16),
            pltpu.VMEM((2, 2, *block), BF16),
            pltpu.VMEM((8, 2, width), BF16),
            pltpu.VMEM((8, 2, width), BF16),
            pltpu.VMEM((8, 2, width), BF16),
            pltpu.VMEM((8, 2, width), BF16),
            pltpu.VMEM((2, 4, 64, hidden), F32),
            pltpu.VMEM(mixed_grad.shape, BF16),
            pltpu.VMEM(merged.shape, BF16),
            pltpu.VMEM(up_weight.shape, F32),
            pltpu.VMEM(down_weight.shape, F32),
            dma((11,)),
            dma((2, 16)),
            dma((2, 4, 5)),
            dma((2, 2)),
            dma((2, 6, 2)),
            dma((2, 3)),
            dma((2, 2)),
            dma((2, 8)),
            dma((2, 2)),
        ],
        compiler_params=pltpu.CompilerParams(
            collective_id=0, has_side_effects=True, vmem_limit_bytes=67043328
        ),
    )(
        merged,
        positions.reshape(1, -1),
        picked.reshape(1, -1),
        router_score.reshape(1, -1),
        mixed_grad,
        up_weight,
        down_weight,
    )
    return pl.pallas_call(
        put_out,
        name="put_out",
        out_shape=tuple(jax.ShapeDtypeStruct(r.shape, r.dtype) for r in results),
        in_specs=[hbm] * 4,
        out_specs=(hbm,) * 4,
        scratch_shapes=[pltpu.VMEM(r.shape, r.dtype) for r in results] + [dma((2, 10))],
        compiler_params=pltpu.CompilerParams(vmem_limit_bytes=67043328),
    )(*results)


def solution(mesh):
    placed = (
        P(VIT_SEQ, "tensor"),
        P(VIT_SEQ),
        P(VIT_SEQ),
        P(VIT_SEQ),
        P("tensor", VIT_SEQ),
        P(VIT_SEQ, "tensor"),
        P(VIT_SEQ, "tensor"),
    )
    return jax.shard_map(
        per_device,
        mesh=mesh,
        in_specs=placed,
        out_specs=(
            P(VIT_SEQ, "tensor"),
            P(VIT_SEQ, "tensor"),
            P("tensor", VIT_SEQ),
            P(VIT_SEQ, "tensor"),
        ),
        check_vma=False,
    )
```
